32 devices in a mesh: cuts: 8 (over z, y), batch: 4 (over x, core).
Axes of the slice: x: 2, y: 2, z: 4, core: 2. Of those that a mesh axis runs over, the one named last changes fastest.
Arguments:
- blocks: bfloat16 [256, 64, 128], P(('cuts', 'batch')), may hold values from -6 to 6
- environments: bfloat16 [256, 64, 128], P(('cuts', 'batch')), may hold values from -0.5 to 0.5
- layers: bfloat16 [8, 64, 128], replicated, may hold values from -0.5 to 0.5
- selectors: bfloat16 [256, 8, 128], P(('cuts', 'batch')), may hold values from -6 to 6
- classes: int32 [32, 8], P(('cuts', 'batch')), may hold values from 1 to 8
- routing: int32 [32, 8], P(('cuts', 'batch')), may hold values from 0 to 7, each once within a row
- left_edges: bfloat16 [64, 128], replicated, may hold values from -0.5 to 0.5
- right_edges: bfloat16 [64, 128], replicated, may hold values from -0.5 to 0.5
- owner_map: int32 [4096], replicated, may hold values from 0 to 4095, each once
Outputs:
- amplitudes: float32 [2, 4096], P(None, ('cuts', 'batch'))
The draws below stay inside these ranges and needn't reach their ends.
Inputs may be any that keep to these rules, and one draw needn't show every extreme that they name: `routing`: each holder's row is a permutation of 0 to 7. `owner_map`: A permutation of the bitstrings.
All inputs are finite; a program needn't handle non-finite values.
Results may differ from the reference program's by a relative error of at most 0.009.
Values may be sent and summed in bfloat16 or wider, within the bound.
A program may use at most 64 MiB of HBM per device.

```python
import jax
import jax.numpy as jnp
from jax import lax

K = 64
HALF = 64
DEPTH = 8
GROUP = 1
SLOTS = 8
HOLDERS = 32
SLICES = 256
BITS = 4096
N_CUTS = 8
N_BATCH = 4


def draw_classes(key, part):
    loaded = jax.random.randint(jax.random.fold_in(key, 11), (HOLDERS, 1), 0, 2)
    strong_levels = jax.random.randint(jax.random.fold_in(key, 12), (HOLDERS, SLOTS), DEPTH // 2 + 1, DEPTH + 1)
    light_levels = jax.random.randint(jax.random.fold_in(key, 13), (HOLDERS, SLOTS), 1, DEPTH // 2)
    return jnp.where(loaded == 1, strong_levels, light_levels).astype(jnp.int32)


def steps_of(stream_key, shape, pieces, smallest, top_value):
    level = 1.0
    for position, parts in pieces:
        heights = jax.random.uniform(jax.random.fold_in(jax.random.fold_in(stream_key, 6), position), (parts,), jnp.float32, smallest / len(pieces), top_value / len(pieces))
        level = level * jnp.repeat(jnp.exp(heights), shape[position] // parts).reshape((-1,) + (1,) * (len(shape) - 1 - position))
    return level


def gaussian(rng, dims, width, most, pieces=(), kind=jnp.bfloat16):
    array = jax.random.normal(rng, dims, jnp.float32) * width
    if len(pieces) > 0:
        array = steps_of(rng, dims, pieces, -0.22, 0.18) * array
    return jnp.clip(array, min=-most, max=most).astype(kind)


def setup_inputs(seed: int = 0) -> dict:
    seeds = jax.random.split(jax.random.key(seed), 10)
    return {
        "blocks": gaussian(seeds[0], (SLICES, K, 2 * K), 1.0, 6.0, ((0, 32),)),
        "environments": gaussian(seeds[1], (SLICES, K, 2 * K), (2 * K) ** -0.5, 0.5, ((0, 32),)),
        "layers": gaussian(seeds[2], (DEPTH, K, 2 * K), (2 * K) ** -0.5, 0.5),
        "selectors": gaussian(seeds[3], (SLICES, DEPTH, 2 * K), 0.7071, 6.0, ((0, 32),)),
        "classes": draw_classes(jax.random.fold_in(seeds[9], 71), 0),
        "routing": jax.vmap(lambda own: jax.random.permutation(own, SLOTS))(jax.random.split(seeds[5], HOLDERS)).reshape((HOLDERS, SLOTS)).astype(jnp.int32),
        "left_edges": gaussian(seeds[6], (K, 2 * HALF), (2 * K) ** -0.5, 0.5),
        "right_edges": gaussian(seeds[7], (K, 2 * HALF), (2 * K) ** -0.5, 0.5),
        "owner_map": jax.random.permutation(seeds[8], BITS).astype(jnp.int32),
    }


def block_form(matrix):
    half_count = matrix.shape[-1] // 2
    real_block = matrix[..., :half_count]
    imag_block = matrix[..., half_count:]
    upper_rows = jnp.concatenate([real_block, imag_block], axis=-1)
    lower_rows = jnp.concatenate([-imag_block, real_block], axis=-1)
    return jnp.concatenate([upper_rows, lower_rows], axis=-2)


def apply_phase(product, factors):
    half_count = product.shape[-1] // 2
    prod_real = product[..., :half_count]
    prod_imag = product[..., half_count:]
    fac_real = factors[..., :half_count].astype(jnp.float32)[:, None, :]
    fac_imag = factors[..., half_count:].astype(jnp.float32)[:, None, :]
    out_real = prod_real * fac_real - prod_imag * fac_imag
    out_imag = prod_real * fac_imag + prod_imag * fac_real
    return jnp.concatenate([out_real, out_imag], axis=-1)


def contract(worked, partners):
    slot_count, bond_width, doubled = worked.shape
    parted = worked.astype(jnp.float32).reshape(slot_count, bond_width, 2, bond_width)
    products = jnp.einsum('sipj,sjk->pik', parted, partners.astype(jnp.float32))
    real_part = products[0, :, :bond_width] - products[1, :, bond_width:]
    imag_part = products[0, :, bond_width:] + products[1, :, :bond_width]
    return real_part, imag_part


def amplitude_table(real_part, imag_part, left_edges, right_edges, owner_map):
    highest = lax.Precision.HIGHEST
    half_count = left_edges.shape[1] // 2
    left_real = left_edges[:, :half_count].astype(jnp.float32)
    left_imag = left_edges[:, half_count:].astype(jnp.float32)
    right_real = right_edges[:, :half_count].astype(jnp.float32)
    right_imag = right_edges[:, half_count:].astype(jnp.float32)
    wave_real = jnp.dot(real_part, right_real, precision=highest) - jnp.dot(imag_part, right_imag, precision=highest)
    wave_imag = jnp.dot(real_part, right_imag, precision=highest) + jnp.dot(imag_part, right_real, precision=highest)
    amp_real = jnp.dot(left_real.T, wave_real, precision=highest) - jnp.dot(left_imag.T, wave_imag, precision=highest)
    amp_imag = jnp.dot(left_real.T, wave_imag, precision=highest) + jnp.dot(left_imag.T, wave_real, precision=highest)
    flattened = jnp.stack([amp_real.reshape(-1), amp_imag.reshape(-1)])
    return flattened[:, owner_map]


def reference(blocks, environments, layers, selectors, classes, routing, left_edges, right_edges, owner_map):
    holders = N_CUTS * N_BATCH
    bond_width = blocks.shape[1]
    tables = block_form(layers).astype(jnp.float32)
    grouped = blocks.reshape(holders, SLOTS, bond_width, 2 * bond_width)
    factor_grid = selectors.reshape(holders, SLOTS, DEPTH, 2 * bond_width)
    partner_grid = environments.reshape(N_CUTS, N_BATCH, SLOTS, bond_width, 2 * bond_width)
    positions = jnp.arange(SLOTS, dtype=jnp.int32)
    targets = positions // GROUP
    within = positions % GROUP

    def one_holder(running, inputs):
        worked, factors, levels, sending, holder = inputs
        cut_index = holder // N_BATCH
        batch_index = holder % N_BATCH
        for layer_index in range(DEPTH):
            product = jnp.einsum('sij,jk->sik', worked.astype(jnp.float32), tables[layer_index])
            updated = apply_phase(product, factors[:, layer_index, :]).astype(jnp.bfloat16)
            worked = jnp.where((levels > layer_index)[:, None, None], updated, worked)
        outgoing = worked[sending]
        partners = partner_grid[targets, batch_index, cut_index * GROUP + within]
        real_part, imag_part = contract(outgoing, partners)
        return (running[0] + real_part, running[1] + imag_part), None

    start_value = (jnp.zeros((bond_width, bond_width), jnp.float32), jnp.zeros((bond_width, bond_width), jnp.float32))
    holder_ids = jnp.arange(holders, dtype=jnp.int32)
    totals, unused = lax.scan(one_holder, start_value, (grouped, factor_grid, classes, routing, holder_ids))
    amp_table = amplitude_table(totals[0], totals[1], left_edges, right_edges, owner_map)
    return amp_table * (SLICES ** -0.5)
```

```python
import functools

import jax
import jax.numpy as jnp
from jax import lax
from jax.experimental import pallas as pl
from jax.experimental.pallas import tpu as pltpu
from jax.sharding import PartitionSpec as P

MESH = pl.DeviceIdType.MESH
UNROLL = 32
GROUP = 8
ROWS = 4
EARLY = 2


def repeat(count, body):
    if count <= UNROLL:
        for step in range(count):
            body(step)
    else:
        lax.fori_loop(0, count, lambda step, carry: (body(step), carry)[1], 0)


def low_half(shape):
    return lax.broadcasted_iota(jnp.int32, shape, len(shape) - 1) < shape[-1] // 2


def swap(x):
    return pltpu.roll(x, x.shape[-1] // 2, x.ndim - 1)


def turn(x):
    swapped = swap(x)
    return jnp.where(low_half(x.shape), -swapped, swapped)


def split(x):
    high = x.astype(jnp.bfloat16)
    return high, (x - high.astype(jnp.float32)).astype(jnp.bfloat16)


def divide(x, by):
    if by & (by - 1) == 0:
        return lax.shift_right_logical(x, jnp.int32(by.bit_length() - 1))
    return lax.div(x, jnp.int32(by))


def kernel(
    sizes,
    blocks_hbm, env_hbm, layers_hbm, sel_hbm, cls_hbm, rout_hbm, left_hbm, right_hbm, own_hbm,
    out_ref,
    blocks, env, layers, sel, cls, rout, left, right, own,
    tables, worked, env_in, hot, left_t, right_t, send, recv,
    in_sem, env_send, env_recv, red_send, red_recv,
):
    cuts, batch = sizes
    holders = cuts * batch
    slots, bond, doubled = blocks.shape
    depth = layers.shape[0]
    member = slots // cuts
    half = doubled // 2
    chunks, unused, width = send.shape
    bits = chunks * width
    per = bits // holders
    mine, row = lax.axis_index("cuts"), lax.axis_index("batch")
    me = mine * batch + row
    f32, bf16 = jnp.float32, jnp.bfloat16

    loads = [
        pltpu.make_async_copy(src, dst, in_sem.at[i])
        for i, (src, dst) in enumerate(
            [
                (layers_hbm, layers), (blocks_hbm, blocks), (sel_hbm, sel), (cls_hbm, cls),
                (env_hbm, env), (own_hbm, own), (left_hbm, left), (right_hbm, right),
                (rout_hbm, rout),
            ]
        )
    ]
    for load in loads:
        load.start()

    barrier = pltpu.get_barrier_semaphore()

    def greet(step):
        other = lax.rem(me + step + 1, holders)
        pl.semaphore_signal(
            barrier, inc=1, device_id=(lax.div(other, batch), lax.rem(other, batch)),
            device_id_type=MESH,
        )

    repeat(holders - 1, greet)

    loads[0].wait()
    for t in range(depth):
        table = layers[t].astype(f32)
        turned = turn(table)
        tables[t, :bond, :doubled] = table.astype(bf16)
        tables[t, :bond, doubled:] = turned.astype(bf16)
        tables[t, bond:, :doubled] = turned.astype(bf16)
        tables[t, bond:, doubled:] = (-table).astype(bf16)
    for load in loads[1:4]:
        load.wait()

    def factors(base, s):
        f = sel[base + s].astype(f32)
        g = swap(f)
        low = low_half(f.shape)
        return jnp.where(low, f, g), jnp.where(low, g, f)

    def advance(base, xs, facs, start, stop):
        xs = list(xs)
        for t in range(start, stop):
            table = tables[t]
            for first in range(0, len(xs), ROWS):
                some = xs[first : first + ROWS]
                both = jnp.dot(
                    jnp.concatenate(some, axis=0), table, preferred_element_type=f32
                )
                for k, x in enumerate(some):
                    s = first + k
                    fr, fi = facs[s]
                    p = both[k * bond : (k + 1) * bond]
                    new = p[:, :doubled] * fr[t : t + 1] + p[:, doubled:] * fi[t : t + 1]
                    active = jnp.full(new.shape, cls[0, base + s], jnp.int32) > t
                    xs[s] = jnp.where(active, new, x.astype(f32)).astype(bf16)
        return xs

    group = min(GROUP, slots)
    xs = [blocks[s] for s in range(group)]
    facs = [factors(0, s) for s in range(group)]
    early = min(EARLY, depth)
    xs = advance(0, xs, facs, 0, early)

    loads[4].wait()
    pl.semaphore_wait(barrier, holders - 1)

    def env_copy(step):
        target = lax.rem(mine + step + 1, cuts)
        return pltpu.make_async_remote_copy(
            src_ref=env.at[pl.ds(target * member, member)],
            dst_ref=env_in.at[step],
            send_sem=env_send.at[step],
            recv_sem=env_recv.at[step],
            device_id=(target, row),
            device_id_type=MESH,
        )

    repeat(cuts - 1, lambda step: env_copy(step).start())

    xs = advance(0, xs, facs, early, depth)
    for s in range(group):
        worked[s] = xs[s]

    def more(index, carry):
        base = index * group
        ys = [blocks[base + s] for s in range(group)]
        ys = advance(base, ys, [factors(base, s) for s in range(group)], 0, depth)
        for s in range(group):
            worked[base + s] = ys[s]
        return carry

    if slots > group:
        lax.fori_loop(1, slots // group, more, 0)

    for load in loads[5:]:
        load.wait()
    r = right[...].astype(f32)
    l = left[...].astype(f32)
    left_t[...] = jnp.concatenate([l, l], axis=0).T.astype(bf16)
    right_t[...] = jnp.concatenate([r, turn(r)], axis=0).T.astype(bf16)
    places = lax.broadcasted_iota(jnp.int32, (half, width), 0)
    for c in range(chunks):
        high = divide(own[c : c + 1, :], half)
        ones = jnp.where(places == high, 1.0, 0.0).astype(bf16)
        hot[:half, c * width : (c + 1) * width] = ones
        hot[half:, c * width : (c + 1) * width] = ones

    zeros = jnp.zeros((bond, doubled), bf16)

    def pair(position, e):
        w = worked[rout[0, position]]
        wide = jnp.concatenate(
            [jnp.concatenate([e, zeros], axis=1), jnp.concatenate([zeros, e], axis=1)], axis=0
        )
        return jnp.dot(w, wide, preferred_element_type=f32)

    acc = jnp.zeros((bond, 2 * doubled), f32)
    for m in range(member):
        acc += pair(mine * member + m, env[mine * member + m])

    def arrive(step, acc):
        env_copy(step).wait_recv()
        source = lax.rem(mine + cuts - step - 1, cuts)
        for m in range(member):
            acc += pair(source * member + m, env_in[step, m])
        return acc

    if cuts - 1 <= UNROLL:
        for step in range(cuts - 1):
            acc = arrive(step, acc)
    else:
        acc = lax.fori_loop(0, cuts - 1, arrive, acc)
    core = acc[:, :doubled] + turn(acc[:, doubled:])

    x = jnp.dot(left_t[...], jnp.concatenate(split(core), axis=0), preferred_element_type=f32)
    v = x[:half] + turn(x[half:])
    y = lax.dot_general(
        right_t[...], jnp.concatenate(split(v), axis=0), (((1,), (1,)), ((), ())),
        preferred_element_type=f32,
    )
    y = y + swap(y)
    high, low = split(y)
    picks = jnp.where(low_half(y.shape), high.astype(f32), low.astype(f32)).astype(bf16)
    for c in range(chunks):
        z = jnp.dot(picks, hot[:, c * width : (c + 1) * width], preferred_element_type=f32)
        place = own[c : c + 1, :]
        mask = places == (place - divide(place, half) * half)
        send[c, 0:1, :] = jnp.sum(jnp.where(mask, z[:half], 0.0), axis=0, keepdims=True)
        send[c, 1:2, :] = jnp.sum(jnp.where(mask, z[half:], 0.0), axis=0, keepdims=True)

    def red_copy(step):
        other = lax.rem(me + step + 1, holders)
        return pltpu.make_async_remote_copy(
            src_ref=send.at[lax.div(other * per, width)],
            dst_ref=recv.at[step],
            send_sem=red_send,
            recv_sem=red_recv,
            device_id=(lax.div(other, batch), lax.rem(other, batch)),
            device_id_type=MESH,
        )

    repeat(holders - 1, lambda step: red_copy(step).start())
    repeat(cuts - 1, lambda step: env_copy(step).wait_send())
    total = send[lax.div(me * per, width)]
    pltpu.make_async_copy(recv, recv, red_recv).wait()
    total = total + jnp.sum(recv[...], axis=0)
    out_ref[...] = total * ((slots * holders) ** (-0.5))
    pltpu.make_async_copy(recv, recv, red_send).wait()


def on_device(sizes, blocks, environments, layers, selectors, classes, routing, left, right, own):
    cuts, batch = sizes
    holders = cuts * batch
    slots, bond, doubled = blocks.shape
    depth = layers.shape[0]
    half = left.shape[1] // 2
    bits = own.shape[0]
    per = bits // holders
    width = max(per, 128)
    chunks = bits // width
    args = (
        blocks, environments, layers, selectors, classes, routing, left, right,
        own.reshape(chunks, width),
    )
    smem = (4, 5)
    out = pl.pallas_call(
        functools.partial(kernel, sizes),
        out_shape=jax.ShapeDtypeStruct((2, width), jnp.float32),
        in_specs=[pl.BlockSpec(memory_space=pl.ANY)] * len(args),
        out_specs=pl.BlockSpec(memory_space=pltpu.VMEM),
        scratch_shapes=[
            (pltpu.SMEM if i in smem else pltpu.VMEM)(a.shape, a.dtype)
            for i, a in enumerate(args)
        ]
        + [
            pltpu.VMEM((depth, 2 * bond, 2 * doubled), jnp.bfloat16),
            pltpu.VMEM((slots, bond, doubled), jnp.bfloat16),
            pltpu.VMEM((cuts - 1, slots // cuts, bond, doubled), jnp.bfloat16),
            pltpu.VMEM((2 * half, bits), jnp.bfloat16),
            pltpu.VMEM((2 * half, 2 * bond), jnp.bfloat16),
            pltpu.VMEM((2 * half, 2 * bond), jnp.bfloat16),
            pltpu.VMEM((chunks, 2, width), jnp.float32),
            pltpu.VMEM((holders - 1, 2, width), jnp.float32),
            pltpu.SemaphoreType.DMA((len(args),)),
            pltpu.SemaphoreType.DMA((cuts - 1,)),
            pltpu.SemaphoreType.DMA((cuts - 1,)),
            pltpu.SemaphoreType.DMA,
            pltpu.SemaphoreType.DMA,
        ],
        compiler_params=pltpu.CompilerParams(collective_id=0, has_side_effects=True),
    )(*args)
    if per < width:
        holder = lax.axis_index("cuts") * batch + lax.axis_index("batch")
        out = lax.dynamic_slice_in_dim(out, lax.rem(holder * per, width), per, 1)
    return out


def solution(mesh):
    placed = (
        P(("cuts", "batch"), None, None),
        P(("cuts", "batch"), None, None),
        P(),
        P(("cuts", "batch"), None, None),
        P(("cuts", "batch"), None),
        P(("cuts", "batch"), None),
        P(),
        P(),
        P(),
    )
    sizes = (mesh.shape["cuts"], mesh.shape["batch"])
    return jax.shard_map(
        functools.partial(on_device, sizes), mesh=mesh, in_specs=placed,
        out_specs=P(None, ("cuts", "batch")), check_vma=False,
    )
```

```python
import functools

import jax
import jax.numpy as jnp
from jax import lax
from jax.experimental import pallas as pl
from jax.experimental.pallas import tpu as pltpu
from jax.sharding import PartitionSpec as P

MESH = pl.DeviceIdType.MESH
UNROLL = 32
GROUP = 8
ROWS = 4
EARLY = 2


def repeat(count, body):
    if count <= UNROLL:
        for step in range(count):
            body(step)
    else:
        lax.fori_loop(0, count, lambda step, carry: (body(step), carry)[1], 0)


def low_half(shape):
    return lax.broadcasted_iota(jnp.int32, shape, len(shape) - 1) < shape[-1] // 2


def swap(x):
    return pltpu.roll(x, x.shape[-1] // 2, x.ndim - 1)


def turn(x):
    swapped = swap(x)
    return jnp.where(low_half(x.shape), -swapped, swapped)


def split(x):
    high = x.astype(jnp.bfloat16)
    return high, (x - high.astype(jnp.float32)).astype(jnp.bfloat16)


def divide(x, by):
    if by & (by - 1) == 0:
        return lax.shift_right_logical(x, jnp.int32(by.bit_length() - 1))
    return lax.div(x, jnp.int32(by))


def kernel(
    sizes,
    blocks_hbm, env_hbm, layers_hbm, sel_hbm, cls_hbm, rout_hbm, left_hbm, right_hbm, own_hbm,
    out_ref,
    blocks, env, layers, sel, cls, rout, left, right, own,
    tables, worked, env_in, hot, left_t, right_t, send, recv,
    in_sem, env_send, env_recv, red_send, red_recv,
):
    cuts, batch = sizes
    holders = cuts * batch
    slots, bond, doubled = blocks.shape
    depth = layers.shape[0]
    member = slots // cuts
    half = doubled // 2
    chunks, unused, width = send.shape
    bits = chunks * width
    per = bits // holders
    mine, row = lax.axis_index("cuts"), lax.axis_index("batch")
    me = mine * batch + row
    f32, bf16 = jnp.float32, jnp.bfloat16

    loads = [
        pltpu.make_async_copy(src, dst, in_sem.at[i])
        for i, (src, dst) in enumerate(
            [
                (layers_hbm, layers), (blocks_hbm, blocks), (sel_hbm, sel), (cls_hbm, cls),
                (env_hbm, env), (own_hbm, own), (left_hbm, left), (right_hbm, right),
                (rout_hbm, rout),
            ]
        )
    ]
    for load in loads:
        load.start()

    barrier = pltpu.get_barrier_semaphore()

    def greet(step):
        other = lax.rem(me + step + 1, holders)
        pl.semaphore_signal(
            barrier, inc=1, device_id=(lax.div(other, batch), lax.rem(other, batch)),
            device_id_type=MESH,
        )

    for step in range(cuts - 1):
        pl.semaphore_signal(barrier, inc=1, device_id=(lax.rem(mine + step + 1, cuts), row), device_id_type=MESH)
    for step in range(batch - 1):
        pl.semaphore_signal(barrier, inc=1, device_id=(mine, lax.rem(row + step + 1, batch)), device_id_type=MESH)

    loads[0].wait()
    for t in range(depth):
        table = layers[t].astype(f32)
        turned = turn(table)
        tables[t, :bond, :doubled] = table.astype(bf16)
        tables[t, :bond, doubled:] = turned.astype(bf16)
        tables[t, bond:, :doubled] = turned.astype(bf16)
        tables[t, bond:, doubled:] = (-table).astype(bf16)
    for load in loads[1:4]:
        load.wait()

    def factors(base, s):
        f = sel[base + s].astype(f32)
        g = swap(f)
        low = low_half(f.shape)
        return jnp.where(low, f, g), jnp.where(low, g, f)

    def advance(base, xs, facs, start, stop):
        xs = list(xs)
        for t in range(start, stop):
            table = tables[t]
            for first in range(0, len(xs), ROWS):
                some = xs[first : first + ROWS]
                both = jnp.dot(
                    jnp.concatenate(some, axis=0), table, preferred_element_type=f32
                )
                for k, x in enumerate(some):
                    s = first + k
                    fr, fi = facs[s]
                    p = both[k * bond : (k + 1) * bond]
                    new = p[:, :doubled] * fr[t : t + 1] + p[:, doubled:] * fi[t : t + 1]
                    active = jnp.full(new.shape, cls[0, base + s], jnp.int32) > t
                    xs[s] = jnp.where(active, new, x.astype(f32)).astype(bf16)
        return xs

    group = min(GROUP, slots)
    xs = [blocks[s] for s in range(group)]
    facs = [factors(0, s) for s in range(group)]
    early = min(EARLY, depth)
    xs = advance(0, xs, facs, 0, early)

    loads[4].wait()
    pl.semaphore_wait(barrier, cuts + batch - 2)

    def env_copy(step):
        target = lax.rem(mine + step + 1, cuts)
        return pltpu.make_async_remote_copy(
            src_ref=env.at[pl.ds(target * member, member)],
            dst_ref=env_in.at[step],
            send_sem=env_send.at[step],
            recv_sem=env_recv.at[step],
            device_id=(target, row),
            device_id_type=MESH,
        )

    repeat(cuts - 1, lambda step: env_copy(step).start())

    xs = advance(0, xs, facs, early, depth)
    for s in range(group):
        worked[s] = xs[s]

    def more(index, carry):
        base = index * group
        ys = [blocks[base + s] for s in range(group)]
        ys = advance(base, ys, [factors(base, s) for s in range(group)], 0, depth)
        for s in range(group):
            worked[base + s] = ys[s]
        return carry

    if slots > group:
        lax.fori_loop(1, slots // group, more, 0)

    for load in loads[5:]:
        load.wait()
    r = right[...].astype(f32)
    l = left[...].astype(f32)
    left_t[...] = jnp.concatenate([l, l], axis=0).T.astype(bf16)
    right_t[...] = jnp.concatenate([r, turn(r)], axis=0).T.astype(bf16)
    places = lax.broadcasted_iota(jnp.int32, (half, width), 0)
    for c in range(chunks):
        high = divide(own[c : c + 1, :], half)
        ones = jnp.where(places == high, 1.0, 0.0).astype(bf16)
        hot[:half, c * width : (c + 1) * width] = ones
        hot[half:, c * width : (c + 1) * width] = ones

    zeros = jnp.zeros((bond, doubled), bf16)

    def pair(position, e):
        w = worked[rout[0, position]]
        wide = jnp.concatenate(
            [jnp.concatenate([e, zeros], axis=1), jnp.concatenate([zeros, e], axis=1)], axis=0
        )
        return jnp.dot(w, wide, preferred_element_type=f32)

    acc = jnp.zeros((bond, 2 * doubled), f32)
    for m in range(member):
        acc += pair(mine * member + m, env[mine * member + m])

    def arrive(step, acc):
        env_copy(step).wait_recv()
        source = lax.rem(mine + cuts - step - 1, cuts)
        for m in range(member):
            acc += pair(source * member + m, env_in[step, m])
        return acc

    if cuts - 1 <= UNROLL:
        for step in range(cuts - 1):
            acc = arrive(step, acc)
    else:
        acc = lax.fori_loop(0, cuts - 1, arrive, acc)
    core = acc[:, :doubled] + turn(acc[:, doubled:])

    x = jnp.dot(left_t[...], jnp.concatenate(split(core), axis=0), preferred_element_type=f32)
    v = x[:half] + turn(x[half:])
    y = lax.dot_general(
        right_t[...], jnp.concatenate(split(v), axis=0), (((1,), (1,)), ((), ())),
        preferred_element_type=f32,
    )
    y = y + swap(y)
    high, low = split(y)
    picks = jnp.where(low_half(y.shape), high.astype(f32), low.astype(f32)).astype(bf16)
    for c in range(chunks):
        z = jnp.dot(picks, hot[:, c * width : (c + 1) * width], preferred_element_type=f32)
        place = own[c : c + 1, :]
        mask = places == (place - divide(place, half) * half)
        send[c, 0:1, :] = jnp.sum(jnp.where(mask, z[:half], 0.0), axis=0, keepdims=True)
        send[c, 1:2, :] = jnp.sum(jnp.where(mask, z[half:], 0.0), axis=0, keepdims=True)

    def red_copy(step):
        other = lax.rem(me + step + 1, holders)
        return pltpu.make_async_remote_copy(
            src_ref=send.at[lax.div(other * per, width)],
            dst_ref=recv.at[step],
            send_sem=red_send,
            recv_sem=red_recv,
            device_id=(lax.div(other, batch), lax.rem(other, batch)),
            device_id_type=MESH,
        )

    repeat(holders - 1, lambda step: red_copy(step).start())
    repeat(cuts - 1, lambda step: env_copy(step).wait_send())
    total = send[lax.div(me * per, width)]
    pltpu.make_async_copy(recv, recv, red_recv).wait()
    total = total + jnp.sum(recv[...], axis=0)
    out_ref[...] = total * ((slots * holders) ** (-0.5))
    pltpu.make_async_copy(recv, recv, red_send).wait()


def on_device(sizes, blocks, environments, layers, selectors, classes, routing, left, right, own):
    cuts, batch = sizes
    holders = cuts * batch
    slots, bond, doubled = blocks.shape
    depth = layers.shape[0]
    half = left.shape[1] // 2
    bits = own.shape[0]
    per = bits // holders
    width = max(per, 128)
    chunks = bits // width
    args = (
        blocks, environments, layers, selectors, classes, routing, left, right,
        own.reshape(chunks, width),
    )
    smem = (4, 5)
    out = pl.pallas_call(
        functools.partial(kernel, sizes),
        out_shape=pltpu.VMEM((2, width), jnp.float32),
        in_specs=[pl.BlockSpec(memory_space=pl.ANY)] * len(args),
        out_specs=pl.BlockSpec(memory_space=pltpu.VMEM),
        scratch_shapes=[
            (pltpu.SMEM if i in smem else pltpu.VMEM)(a.shape, a.dtype)
            for i, a in enumerate(args)
        ]
        + [
            pltpu.VMEM((depth, 2 * bond, 2 * doubled), jnp.bfloat16),
            pltpu.VMEM((slots, bond, doubled), jnp.bfloat16),
            pltpu.VMEM((cuts - 1, slots // cuts, bond, doubled), jnp.bfloat16),
            pltpu.VMEM((2 * half, bits), jnp.bfloat16),
            pltpu.VMEM((2 * half, 2 * bond), jnp.bfloat16),
            pltpu.VMEM((2 * half, 2 * bond), jnp.bfloat16),
            pltpu.VMEM((chunks, 2, width), jnp.float32),
            pltpu.VMEM((holders - 1, 2, width), jnp.float32),
            pltpu.SemaphoreType.DMA((len(args),)),
            pltpu.SemaphoreType.DMA((cuts - 1,)),
            pltpu.SemaphoreType.DMA((cuts - 1,)),
            pltpu.SemaphoreType.DMA,
            pltpu.SemaphoreType.DMA,
        ],
        compiler_params=pltpu.CompilerParams(collective_id=0, has_side_effects=True),
    )(*args)
    if per < width:
        holder = lax.axis_index("cuts") * batch + lax.axis_index("batch")
        out = lax.dynamic_slice_in_dim(out, lax.rem(holder * per, width), per, 1)
    return out


def solution(mesh):
    placed = (
        P(("cuts", "batch"), None, None),
        P(("cuts", "batch"), None, None),
        P(),
        P(("cuts", "batch"), None, None),
        P(("cuts", "batch"), None),
        P(("cuts", "batch"), None),
        P(),
        P(),
        P(),
    )
    sizes = (mesh.shape["cuts"], mesh.shape["batch"])
    return jax.shard_map(
        functools.partial(on_device, sizes), mesh=mesh, in_specs=placed,
        out_specs=P(None, ("cuts", "batch")), check_vma=False,
    )
```

```python
import functools

import jax
import jax.numpy as jnp
from jax import lax
from jax.experimental import pallas as pl
from jax.experimental.pallas import tpu as pltpu
from jax.sharding import PartitionSpec as P

MESH = pl.DeviceIdType.MESH
UNROLL = 32
GROUP = 8
ROWS = 4
EARLY = 2


def repeat(count, body):
    if count <= UNROLL:
        for step in range(count):
            body(step)
    else:
        lax.fori_loop(0, count, lambda step, carry: (body(step), carry)[1], 0)


def low_half(shape):
    return lax.broadcasted_iota(jnp.int32, shape, len(shape) - 1) < shape[-1] // 2


def swap(x):
    return pltpu.roll(x, x.shape[-1] // 2, x.ndim - 1)


def turn(x):
    swapped = swap(x)
    return jnp.where(low_half(x.shape), -swapped, swapped)


def split(x):
    high = x.astype(jnp.bfloat16)
    return high, (x - high.astype(jnp.float32)).astype(jnp.bfloat16)


def divide(x, by):
    if by & (by - 1) == 0:
        return lax.shift_right_logical(x, jnp.int32(by.bit_length() - 1))
    return lax.div(x, jnp.int32(by))


def kernel(
    sizes,
    blocks_hbm, env_hbm, layers_hbm, sel_hbm, cls_hbm, rout_hbm, left_hbm, right_hbm, own_hbm,
    out_ref,
    blocks, env, layers, sel, cls, rout, left, right, own,
    tables, worked, folded, env_in, hot, left_t, right_t, send, recv,
    in_sem, env_send, env_recv, red_send, red_recv,
):
    cuts, batch = sizes
    holders = cuts * batch
    slots, bond, doubled = blocks.shape
    depth = layers.shape[0]
    member = slots // cuts
    half = doubled // 2
    chunks, unused, width = send.shape
    bits = chunks * width
    per = bits // holders
    mine, row = lax.axis_index("cuts"), lax.axis_index("batch")
    me = mine * batch + row
    f32, bf16 = jnp.float32, jnp.bfloat16

    loads = [
        pltpu.make_async_copy(src, dst, in_sem.at[i])
        for i, (src, dst) in enumerate(
            [
                (layers_hbm, layers), (blocks_hbm, blocks), (sel_hbm, sel), (cls_hbm, cls),
                (env_hbm, env), (own_hbm, own), (left_hbm, left), (right_hbm, right),
                (rout_hbm, rout),
            ]
        )
    ]
    for load in loads:
        load.start()

    barrier = pltpu.get_barrier_semaphore()

    def greet(step):
        other = lax.rem(me + step + 1, holders)
        pl.semaphore_signal(
            barrier, inc=1, device_id=(lax.div(other, batch), lax.rem(other, batch)),
            device_id_type=MESH,
        )

    for step in range(cuts - 1):
        pl.semaphore_signal(barrier, inc=1, device_id=(lax.rem(mine + step + 1, cuts), row), device_id_type=MESH)
    for step in range(batch - 1):
        pl.semaphore_signal(barrier, inc=1, device_id=(mine, lax.rem(row + step + 1, batch)), device_id_type=MESH)

    loads[0].wait()
    for t in range(depth):
        table = layers[t].astype(f32)
        turned = turn(table)
        tables[t, :bond, :doubled] = table.astype(bf16)
        tables[t, :bond, doubled:] = turned.astype(bf16)
        tables[t, bond:, :doubled] = turned.astype(bf16)
        tables[t, bond:, doubled:] = (-table).astype(bf16)
    for load in loads[1:4]:
        load.wait()

    def factors(base, s):
        f = sel[base + s].astype(f32)
        g = swap(f)
        low = low_half(f.shape)
        return jnp.where(low, f, g), jnp.where(low, g, f)

    def advance(base, xs, facs, start, stop):
        xs = list(xs)
        for t in range(start, stop):
            table = tables[t]
            for first in range(0, len(xs), ROWS):
                some = xs[first : first + ROWS]
                both = jnp.dot(
                    jnp.concatenate(some, axis=0), table, preferred_element_type=f32
                )
                for k, x in enumerate(some):
                    s = first + k
                    fr, fi = facs[s]
                    p = both[k * bond : (k + 1) * bond]
                    new = p[:, :doubled] * fr[t : t + 1] + p[:, doubled:] * fi[t : t + 1]
                    active = jnp.full(new.shape, cls[0, base + s], jnp.int32) > t
                    xs[s] = jnp.where(active, new, x.astype(f32)).astype(bf16)
        return xs

    group = min(GROUP, slots)
    xs = [blocks[s] for s in range(group)]
    facs = [factors(0, s) for s in range(group)]
    early = min(EARLY, depth)
    xs = advance(0, xs, facs, 0, early)

    loads[4].wait()
    pl.semaphore_wait(barrier, cuts + batch - 2)

    def env_copy(step):
        target = lax.rem(mine + step + 1, cuts)
        return pltpu.make_async_remote_copy(
            src_ref=env.at[pl.ds(target * member, member)],
            dst_ref=env_in.at[step],
            send_sem=env_send.at[step],
            recv_sem=env_recv.at[step],
            device_id=(target, row),
            device_id_type=MESH,
        )

    repeat(cuts - 1, lambda step: env_copy(step).start())

    xs = advance(0, xs, facs, early, depth)
    for s in range(group):
        worked[s] = xs[s]

    def more(index, carry):
        base = index * group
        ys = [blocks[base + s] for s in range(group)]
        ys = advance(base, ys, [factors(base, s) for s in range(group)], 0, depth)
        for s in range(group):
            worked[base + s] = ys[s]
        return carry

    if slots > group:
        lax.fori_loop(1, slots // group, more, 0)

    for load in loads[5:]:
        load.wait()
    r = right[...].astype(f32)
    l = left[...].astype(f32)
    left_t[...] = l.T.astype(bf16)
    right_t[...] = jnp.concatenate([r, turn(r)], axis=0).T.astype(bf16)

    def fold(s):
        x = jnp.dot(left_t[...], worked[s], preferred_element_type=f32)
        high, low = split(x[:half] + turn(x[half:]))
        folded[s, :, :doubled] = high
        folded[s, :, doubled:] = low

    repeat(slots, fold)
    places = lax.broadcasted_iota(jnp.int32, (half, width), 0)
    for c in range(chunks):
        high = divide(own[c : c + 1, :], half)
        ones = jnp.where(places == high, 1.0, 0.0).astype(bf16)
        hot[:half, c * width : (c + 1) * width] = ones
        hot[half:, c * width : (c + 1) * width] = ones

    zeros = jnp.zeros((bond, doubled), bf16)

    def pair(position, e):
        w = folded[rout[0, position]]
        wide = jnp.concatenate(
            [jnp.concatenate([e, zeros], axis=1), jnp.concatenate([zeros, e], axis=1)], axis=0
        )
        twice = jnp.concatenate([wide, wide], axis=0)
        return jnp.dot(w, twice, preferred_element_type=f32)

    acc = jnp.zeros((half, 2 * doubled), f32)
    for m in range(member):
        acc += pair(mine * member + m, env[mine * member + m])

    def arrive(step, acc):
        env_copy(step).wait_recv()
        source = lax.rem(mine + cuts - step - 1, cuts)
        for m in range(member):
            acc += pair(source * member + m, env_in[step, m])
        return acc

    if cuts - 1 <= UNROLL:
        for step in sorted(range(cuts - 1), key=lambda s: min(s, cuts - 2 - s)):
            acc = arrive(step, acc)
    else:
        acc = lax.fori_loop(0, cuts - 1, arrive, acc)
    v = acc[:, :doubled] + turn(acc[:, doubled:])
    y = lax.dot_general(
        right_t[...], jnp.concatenate(split(v), axis=0), (((1,), (1,)), ((), ())),
        preferred_element_type=f32,
    )
    y = y + swap(y)
    high, low = split(y)
    picks = jnp.where(low_half(y.shape), high.astype(f32), low.astype(f32)).astype(bf16)
    for c in range(chunks):
        z = jnp.dot(picks, hot[:, c * width : (c + 1) * width], preferred_element_type=f32)
        place = own[c : c + 1, :]
        mask = places == (place - divide(place, half) * half)
        send[c, 0:1, :] = jnp.sum(jnp.where(mask, z[:half], 0.0), axis=0, keepdims=True)
        send[c, 1:2, :] = jnp.sum(jnp.where(mask, z[half:], 0.0), axis=0, keepdims=True)

    def red_copy(step):
        other = lax.rem(me + step + 1, holders)
        return pltpu.make_async_remote_copy(
            src_ref=send.at[lax.div(other * per, width)],
            dst_ref=recv.at[step],
            send_sem=red_send,
            recv_sem=red_recv,
            device_id=(lax.div(other, batch), lax.rem(other, batch)),
            device_id_type=MESH,
        )

    repeat(holders - 1, lambda step: red_copy(step).start())
    repeat(cuts - 1, lambda step: env_copy(step).wait_send())
    total = send[lax.div(me * per, width)]
    pltpu.make_async_copy(recv, recv, red_recv).wait()
    total = total + jnp.sum(recv[...], axis=0)
    out_ref[...] = total * ((slots * holders) ** (-0.5))
    pltpu.make_async_copy(recv, recv, red_send).wait()


def on_device(sizes, blocks, environments, layers, selectors, classes, routing, left, right, own):
    cuts, batch = sizes
    holders = cuts * batch
    slots, bond, doubled = blocks.shape
    depth = layers.shape[0]
    half = left.shape[1] // 2
    bits = own.shape[0]
    per = bits // holders
    width = max(per, 128)
    chunks = bits // width
    args = (
        blocks, environments, layers, selectors, classes, routing, left, right,
        own.reshape(chunks, width),
    )
    smem = (4, 5)
    out = pl.pallas_call(
        functools.partial(kernel, sizes),
        out_shape=pltpu.VMEM((2, width), jnp.float32),
        in_specs=[pl.BlockSpec(memory_space=pl.ANY)] * len(args),
        out_specs=pl.BlockSpec(memory_space=pltpu.VMEM),
        scratch_shapes=[
            (pltpu.SMEM if i in smem else pltpu.VMEM)(a.shape, a.dtype)
            for i, a in enumerate(args)
        ]
        + [
            pltpu.VMEM((depth, 2 * bond, 2 * doubled), jnp.bfloat16),
            pltpu.VMEM((slots, bond, doubled), jnp.bfloat16),
            pltpu.VMEM((slots, half, 2 * doubled), jnp.bfloat16),
            pltpu.VMEM((cuts - 1, slots // cuts, bond, doubled), jnp.bfloat16),
            pltpu.VMEM((2 * half, bits), jnp.bfloat16),
            pltpu.VMEM((2 * half, bond), jnp.bfloat16),
            pltpu.VMEM((2 * half, 2 * bond), jnp.bfloat16),
            pltpu.VMEM((chunks, 2, width), jnp.float32),
            pltpu.VMEM((holders - 1, 2, width), jnp.float32),
            pltpu.SemaphoreType.DMA((len(args),)),
            pltpu.SemaphoreType.DMA((cuts - 1,)),
            pltpu.SemaphoreType.DMA((cuts - 1,)),
            pltpu.SemaphoreType.DMA,
            pltpu.SemaphoreType.DMA,
        ],
        compiler_params=pltpu.CompilerParams(collective_id=0, has_side_effects=True),
    )(*args)
    if per < width:
        holder = lax.axis_index("cuts") * batch + lax.axis_index("batch")
        out = lax.dynamic_slice_in_dim(out, lax.rem(holder * per, width), per, 1)
    return out


def solution(mesh):
    placed = (
        P(("cuts", "batch"), None, None),
        P(("cuts", "batch"), None, None),
        P(),
        P(("cuts", "batch"), None, None),
        P(("cuts", "batch"), None),
        P(("cuts", "batch"), None),
        P(),
        P(),
        P(),
    )
    sizes = (mesh.shape["cuts"], mesh.shape["batch"])
    return jax.shard_map(
        functools.partial(on_device, sizes), mesh=mesh, in_specs=placed,
        out_specs=P(None, ("cuts", "batch")), check_vma=False,
    )
```
